32 devices in a mesh: row: 2 (over x), col: 16 (over z, y, core).
Axes of the slice: x: 2, y: 2, z: 4, core: 2. Of those that a mesh axis runs over, the one named last changes fastest.
Arguments:
- tokens: bfloat16 [512, 4608], P('col', 'row'), may hold values from -6 to 6
- pre_gain: float32 [2, 4608], P(None, 'row'), may hold values from -0.6 to 0.6
- post_gain: float32 [2, 4608], P(None, 'row'), may hold values from -0.6 to 0.6
- gate_weight: bfloat16 [2, 4608, 36864], P(None, ('row', 'col')), may hold values from -0.09375 to 0.09375
- up_weight: bfloat16 [2, 4608, 36864], P(None, ('row', 'col')), may hold values from -0.09375 to 0.09375
- down_weight: bfloat16 [2, 36864, 4608], P(None, ('row', 'col')), may hold values from -0.13541667 to 0.13541667
Outputs:
- stream: bfloat16 [512, 4608], P('col', 'row')
The draws below stay inside these ranges and needn't reach their ends.
All inputs are finite; a program needn't handle non-finite values.
Results may differ from the reference program's by a relative error of at most 0.019.
Values may be sent and summed in bfloat16 or wider, within the bound.
A program may use at most 256 MiB of HBM per device.

```python
import math
import jax
import jax.numpy as jnp
from jax import lax

D = 4608
FF = 36864
LAYERS = 2
TOKENS = 512


def draw_down_weight(key, part):
    key_main = jax.random.fold_in(key, 11)
    key_rough = jax.random.fold_in(key, 12)
    entries = jax.random.truncated_normal(key_main, -6.0, 6.0, (LAYERS, FF, D), jnp.float32)
    low_end = 0.5
    high_end = 2.0
    ramp = jnp.linspace(math.log(low_end), math.log(high_end), D, dtype=jnp.float32)
    rough = jax.random.uniform(key_rough, (LAYERS, 1, D), jnp.float32, math.log(0.7), math.log(1.4))
    scales = jnp.exp(ramp[None, None, :] + rough)
    return (entries * scales * FF ** (-0.5)).astype(jnp.bfloat16)


def block_levels(own_key, shape, shards, least, top_value):
    loudness = 1.0
    for axis_at, blocks in shards:
        draws = jax.random.uniform(jax.random.fold_in(jax.random.fold_in(own_key, 6), axis_at), (blocks,), jnp.float32, least / len(shards), top_value / len(shards))
        loudness = loudness * jnp.repeat(jnp.exp(draws), shape[axis_at] // blocks).reshape((-1,) + (1,) * (len(shape) - 1 - axis_at))
    return loudness


def bell_draw(stream_key, extent, scale, most, pieces=(), held_as=jnp.bfloat16):
    drawn = jax.random.normal(stream_key, extent, jnp.float32) * scale
    if len(pieces) > 0:
        drawn = block_levels(stream_key, extent, pieces, -0.22, 0.18) * drawn
    return jnp.clip(drawn, min=-most, max=most).astype(held_as)


def setup_inputs(seed: int = 0) -> dict:
    seeds = jax.random.split(jax.random.key(seed), 7)
    return {
        "tokens": bell_draw(seeds[0], (TOKENS, D), 1.0, 6.0, ((0, 16), (1, 2))),
        "pre_gain": jnp.clip(jax.random.uniform(seeds[1], (LAYERS, D), jnp.float32, -0.6, 0.6) * block_levels(seeds[1], (LAYERS, D), ((1, 2),), -0.4, 0.0), -0.6, 0.6),
        "post_gain": jnp.clip(jax.random.uniform(seeds[2], (LAYERS, D), jnp.float32, -0.6, 0.6) * block_levels(seeds[2], (LAYERS, D), ((1, 2),), -0.4, 0.0), -0.6, 0.6),
        "gate_weight": bell_draw(seeds[3], (LAYERS, D, FF), D ** -0.5, 0.09375, ((1, 32),)),
        "up_weight": bell_draw(seeds[4], (LAYERS, D, FF), D ** -0.5, 0.09375, ((1, 32),)),
        "down_weight": draw_down_weight(jax.random.fold_in(seeds[6], 71), 0),
    }


norm_eps = 1e-06

def reference(tokens, pre_gain, post_gain, gate_weight, up_weight, down_weight):
    current = tokens
    for layer_index in range(LAYERS):
        values = current.astype(jnp.float32)
        mean_sq = lax.optimization_barrier(jnp.mean(values * values, axis=1, keepdims=True))
        normed = (values * lax.rsqrt(mean_sq + norm_eps) * (1.0 + pre_gain[layer_index])[None, :]).astype(jnp.bfloat16)
        gate = jnp.dot(normed, gate_weight[layer_index], preferred_element_type=jnp.float32)
        up_proj = jnp.dot(normed, up_weight[layer_index], preferred_element_type=jnp.float32)
        hidden = (jax.nn.gelu(gate, approximate=True) * up_proj).astype(jnp.bfloat16)
        branch = jnp.dot(hidden, down_weight[layer_index], preferred_element_type=jnp.float32)
        branch_sq = lax.optimization_barrier(jnp.mean(branch * branch, axis=1, keepdims=True))
        post = branch * lax.rsqrt(branch_sq + norm_eps) * (1.0 + post_gain[layer_index])[None, :]
        current = (values + post).astype(jnp.bfloat16)
    return current
```

```python
import functools

import jax
import jax.numpy as jnp
from jax import lax
from jax.experimental import pallas as pl
from jax.experimental.pallas import tpu as pltpu
from jax.sharding import PartitionSpec as P

norm_eps = 1e-06
AXES = ("row", "col")
MESH = pl.DeviceIdType.MESH
LANES = 128

AHEAD = 6
EXTRA = 8
LAG = 3


def div(a, b):
    return lax.div(a, jnp.int32(b))


def rem(a, b):
    return lax.rem(a, jnp.int32(b))


def fits(row_count, col_count, shapes):
    (_, width), (_, rows, hidden), (_, block, _) = shapes
    return (
        row_count == 2
        and col_count % 4 == 0
        and rows % 16 == 0
        and block % LANES == 0
        and width % LANES == 0
    )


def fused_kernel(
    dims,
    tokens_ref,
    pre_ref,
    post_ref,
    gate_ref,
    up_ref,
    down_ref,
    out_ref,
    wbuf,
    vals,
    ssend,
    srecv,
    nstage,
    nrecv,
    lhs,
    tile,
    acc,
    ysend,
    yrecv,
    zsend,
    zrecv,
    hidden,
    dtile,
    csend,
    crecv,
    bacc,
    xs,
    xr,
    ys,
    yr,
    zs,
    zr,
    branch,
    ssend_sem,
    srecv_sem,
    nsend_sem,
    nrecv_sem,
    wsend_sem,
    wrecv_sem,
    tile_sem,
    ysend_sem,
    yrecv_sem,
    zsend_sem,
    zrecv_sem,
    dtile_sem,
    bsend_sem,
    brecv_sem,
):
    layers, planes, chunks, steps = dims
    cols = planes * 4
    own_tokens, own_width = tokens_ref.shape
    model_width = 2 * own_width
    rows = gate_ref.shape[1]
    block = down_ref.shape[1]
    kpad = nstage.shape[2]
    units = planes * chunks
    total_units = layers * units
    slots = ysend.shape[0]
    acc_slots = acc.shape[0]
    half = cols // 2 * own_tokens
    quarter = half // 2
    piece = xs.shape[2]

    x = lax.axis_index("row")
    col = lax.axis_index("col")
    z, y, c = div(col, 4), rem(div(col, 2), 2), rem(col, 2)

    def place(px, pz, py, pc):
        return (px, pz * 4 + py * 2 + pc)

    def send(src, dst, send_sem, recv_sem, to):
        copy = pltpu.make_async_remote_copy(
            src_ref=src,
            dst_ref=dst,
            send_sem=send_sem,
            recv_sem=recv_sem,
            device_id=to,
            device_id_type=MESH,
        )
        copy.start()

    def wait_bytes(ref, sem):
        pltpu.make_async_copy(ref, ref, sem).wait()

    def offset(value, size):
        return pl.multiple_of(value, size)

    barrier = pltpu.get_barrier_semaphore()

    def greet(i, carry):
        other = rem(x * cols + col + i, 2 * cols)
        pl.semaphore_signal(
            barrier, inc=1, device_id=(div(other, cols), rem(other, cols)), device_id_type=MESH
        )
        return carry

    lax.fori_loop(1, 2 * cols, greet, 0)
    pl.semaphore_wait(barrier, 2 * cols - 1)

    def unit_of(u):
        shift = planes - 1 - div(u, chunks)
        j = rem(u, chunks)
        return shift, j, rem(j, 2)

    def issue_weights(g):
        layer = div(g, units)
        shift, j, s = unit_of(rem(g, units))
        pz = rem(z + shift, planes)
        for da, dc in ((0, 1), (1, 0), (1, 1)):
            px = rem(x + da * (1 - s), 2)
            py = rem(y + da * s, 2)
            pc = rem(c + dc, 2)
            slot = 2 * da + dc - 1
            for db in range(2):
                ox = rem(px + db * s, 2)
                oy = rem(py + db * (1 - s), 2)
                owner = ox * cols + pz * 4 + oy * 2 + pc
                start = offset(owner * block + j * LANES, LANES)
                for which, ref in enumerate((gate_ref, up_ref)):
                    send(
                        ref.at[layer, :, pl.ds(start, LANES)],
                        wbuf.at[g, slot, :, pl.ds((2 * db + which) * LANES, LANES)],
                        wsend_sem.at[g],
                        wrecv_sem.at[g],
                        place(px, z, py, pc),
                    )

    def issue_if(g):
        @pl.when(g < total_units)
        def _():
            issue_weights(g)

    def load_tile(g, slot):
        layer = div(g, units)
        shift, j, s = unit_of(rem(g, units))
        pz = rem(z + shift, planes)
        for db in range(2):
            ox = rem(x + db * s, 2)
            oy = rem(y + db * (1 - s), 2)
            owner = ox * cols + pz * 4 + oy * 2 + c
            start = offset(owner * block + j * LANES, LANES)
            for which, ref in enumerate((gate_ref, up_ref)):
                pltpu.make_async_copy(
                    ref.at[layer, :, pl.ds(start, LANES)],
                    tile.at[
                        slot,
                        pl.ds(offset(c * rows, 16), rows),
                        pl.ds((2 * db + which) * LANES, LANES),
                    ],
                    tile_sem.at[slot],
                ).start()
        for da, dc in ((0, 1), (1, 0), (1, 1)):
            pc = rem(c + dc, 2)
            pltpu.make_async_copy(
                wbuf.at[g, 2 * da + dc - 1],
                tile.at[slot, pl.ds(offset(da * kpad + pc * rows, 16), rows), :],
                tile_sem.at[slot],
            ).start()

    def wait_tile(slot):
        wait_bytes(tile.at[slot, pl.ds(0, 4 * rows), :], tile_sem.at[slot])

    def load_down(layer, k, slot):
        for i in range(2):
            px = rem(x + i, 2)
            pltpu.make_async_copy(
                down_ref.at[layer, :, pl.ds(offset(px * own_width + k * piece, LANES), piece)],
                dtile.at[slot, :, pl.ds(i * piece, piece)],
                dtile_sem.at[slot],
            ).start()

    def add_over_rows(index, squares):
        ssend[index] = jnp.broadcast_to(squares, ssend.shape[1:])
        send(
            ssend.at[index], srecv.at[index], ssend_sem.at[index], srecv_sem.at[index], (1 - x, col)
        )
        wait_bytes(srecv.at[index], srecv_sem.at[index])
        wait_bytes(ssend.at[index], ssend_sem.at[index])
        return squares + srecv[index][:, 0:1]

    for g in range(AHEAD):
        issue_weights(jnp.int32(g))

    nstage[...] = jnp.zeros_like(nstage)
    tile[...] = jnp.zeros_like(tile)
    vals[...] = tokens_ref[...].astype(jnp.float32)

    def layer_step(layer, carry):
        load_down(layer, 0, 0)
        load_down(layer, 1, 1)
        values = vals[...]
        squares = add_over_rows(2 * layer, jnp.sum(values * values, axis=1, keepdims=True))
        scale = lax.rsqrt(squares / model_width + norm_eps)
        normed = values * scale * (1.0 + pre_ref[layer])
        width = 2 * rows
        for q in range(own_width // width):
            nstage[q, :, 0:width] = normed[:, q * width : (q + 1) * width].astype(jnp.bfloat16)

        here = offset((c * (cols // 2) + y * planes + z) * own_tokens, own_tokens)
        lines = pl.ds(here, own_tokens)

        def scatter(i, carry):
            other = rem(col + i, cols)
            oz, oy = div(other, 4), rem(div(other, 2), 2)
            for slot, block_at in ((0, oz * 2 + oy), (2, oz * 2 + 1 - oy)):
                send(
                    nstage.at[block_at],
                    nrecv.at[slot, lines, :],
                    nsend_sem.at[slot],
                    nrecv_sem.at[slot],
                    (x, other),
                )
            return carry

        def cross(i, carry):
            other = rem(col + i, cols)
            oz, oy = div(other, 4), rem(div(other, 2), 2)
            send(
                nstage.at[oz * 2 + oy],
                nrecv.at[1, lines, :],
                nsend_sem.at[1],
                nrecv_sem.at[1],
                (1 - x, other),
            )
            return carry

        lax.fori_loop(0, cols, cross, 0)
        lax.fori_loop(1, cols, scatter, 0)
        nrecv[0, lines, :] = nstage[z * 2 + y]
        nrecv[2, lines, :] = nstage[z * 2 + 1 - y]
        most = pl.ds(0, (cols - 1) * own_tokens)
        for slot in (1, 0, 2):
            part = nrecv.at[slot] if slot == 1 else nrecv.at[slot, most, :]
            wait_bytes(part, nrecv_sem.at[slot])
        for slot in (1, 0, 2):
            part = nrecv.at[slot] if slot == 1 else nrecv.at[slot, most, :]
            wait_bytes(part, nsend_sem.at[slot])
        for s in range(2):
            lhs[s, :, 0:kpad] = nrecv[0]
            lhs[s, :, kpad : 2 * kpad] = nrecv[1 + s]

        def unit_step(u, carry):
            g = layer * units + u
            slot = rem(u, 2)

            @pl.when(u < units)
            def _():
                issue_if(g + AHEAD + EXTRA * layer)
                wait_bytes(wbuf.at[g], wrecv_sem.at[g])
                load_tile(g, slot)

            v = u - LAG

            @pl.when(v >= 0)
            def _():
                shift, j, s = unit_of(v)
                wait_bytes(yrecv.at[v], yrecv_sem.at[v])
                summed = acc[rem(v, acc_slots)] + yrecv[v].astype(jnp.float32)

                @pl.when(shift > 0)
                def _():
                    out = rem(v, slots)

                    @pl.when(v >= slots)
                    def _():
                        wait_bytes(zsend.at[out], zsend_sem.at[out])

                    zsend[out] = summed.astype(jnp.bfloat16)
                    at = (shift - 1) * chunks + j
                    send(
                        zsend.at[out],
                        zrecv.at[at],
                        zsend_sem.at[out],
                        zrecv_sem.at[at],
                        place(x, rem(z + shift, planes), y, c),
                    )

                @pl.when(shift == 0)
                def _():
                    whole = summed
                    for i in range(planes - 1):
                        at = i * chunks + j
                        wait_bytes(zrecv.at[at], zrecv_sem.at[at])
                        whole = whole + zrecv[at].astype(jnp.float32)
                    gate, up_proj = whole[:, :LANES], whole[:, LANES:]
                    hidden[:, pl.ds(offset(j * LANES, LANES), LANES)] = (
                        jax.nn.gelu(gate, approximate=True) * up_proj
                    ).astype(jnp.bfloat16)

            @pl.when(u < units)
            def _():
                shift, j, s = unit_of(u)
                wait_tile(slot)
                part = jnp.dot(lhs[s], tile[slot], preferred_element_type=jnp.float32)
                out = rem(u, slots)

                @pl.when(u >= slots)
                def _():
                    wait_bytes(ysend.at[out], ysend_sem.at[out])

                ysend[out] = part[:, 2 * LANES :].astype(jnp.bfloat16)
                acc[rem(u, acc_slots)] = part[:, : 2 * LANES]
                send(
                    ysend.at[out],
                    yrecv.at[u],
                    ysend_sem.at[out],
                    yrecv_sem.at[u],
                    place(rem(x + s, 2), z, rem(y + 1 - s, 2), c),
                )

            return carry

        lax.fori_loop(0, units + LAG, unit_step, 0)
        for out in range(min(slots, units)):
            wait_bytes(ysend.at[out], ysend_sem.at[out])
        for out in range(min(slots, units - chunks)):
            wait_bytes(zsend.at[out], zsend_sem.at[out])

        own_half = pl.ds(offset(c * half, half), half)
        far_half = pl.ds(offset((1 - c) * half, half), half)
        own_quarter = pl.ds(offset(y * quarter, quarter), quarter)
        far_quarter = pl.ds(offset((1 - y) * quarter, quarter), quarter)
        own_lines = pl.ds(offset(z * own_tokens, own_tokens), own_tokens)

        def multiply(k):
            slot = k % 2
            wait_bytes(dtile.at[slot], dtile_sem.at[slot])
            csend[k] = jnp.dot(
                hidden[far_half, :], dtile[slot], preferred_element_type=jnp.float32
            ).astype(jnp.bfloat16)
            send(
                csend.at[k], crecv.at[k], bsend_sem.at[0, k], brecv_sem.at[0, k], place(x, z, y, 1 - c)
            )
            bacc[k] = jnp.dot(hidden[own_half, :], dtile[slot], preferred_element_type=jnp.float32)
            if k + 2 < steps:
                load_down(layer, k + 2, slot)

        def over_x(k):
            wait_bytes(crecv.at[k], brecv_sem.at[0, k])
            summed = bacc[k] + crecv[k].astype(jnp.float32)
            xs[k] = summed[:, piece:].astype(jnp.bfloat16)
            send(
                xs.at[k], xr.at[k], bsend_sem.at[1, k], brecv_sem.at[1, k], place(1 - x, z, y, c)
            )
            bacc[k, :, 0:piece] = summed[:, :piece]

        def over_y(k):
            wait_bytes(xr.at[k], brecv_sem.at[1, k])
            bacc[k, :, 0:piece] = bacc[k, :, 0:piece] + xr[k].astype(jnp.float32)
            ys[k] = bacc[k, far_quarter, 0:piece].astype(jnp.bfloat16)
            send(
                ys.at[k], yr.at[k], bsend_sem.at[2, k], brecv_sem.at[2, k], place(x, z, 1 - y, c)
            )

        def over_z(k):
            wait_bytes(yr.at[k], brecv_sem.at[2, k])
            summed = bacc[k, own_quarter, 0:piece] + yr[k].astype(jnp.float32)
            bacc[k, 0:quarter, 0:piece] = summed
            zs[k] = summed.astype(jnp.bfloat16)
            for shift in range(1, planes):
                pz = rem(z + shift, planes)
                send(
                    zs.at[k, pl.ds(offset(pz * own_tokens, own_tokens), own_tokens), :],
                    zr.at[k, shift - 1],
                    bsend_sem.at[2 + shift, k],
                    brecv_sem.at[2 + shift, k],
                    place(x, pz, y, c),
                )

        def finish(k):
            total = bacc[k, own_lines, 0:piece]
            for shift in range(1, planes):
                wait_bytes(zr.at[k, shift - 1], brecv_sem.at[2 + shift, k])
                total = total + zr[k, shift - 1].astype(jnp.float32)
            branch[:, k * piece : (k + 1) * piece] = total

        stages = (multiply, over_x, over_y, over_z, finish)
        for t in range(steps + len(stages) - 1):
            for lag, stage in enumerate(stages):
                if 0 <= t - lag < steps:
                    stage(t - lag)
            if t < EXTRA:
                issue_if((layer + 1) * units + AHEAD + EXTRA * layer + t)
        for t in range(steps + len(stages) - 1, EXTRA):
            issue_if((layer + 1) * units + AHEAD + EXTRA * layer + t)
        for k in range(steps):
            wait_bytes(csend.at[k], bsend_sem.at[0, k])
            wait_bytes(xs.at[k], bsend_sem.at[1, k])
            wait_bytes(ys.at[k], bsend_sem.at[2, k])
            for shift in range(1, planes):
                wait_bytes(zr.at[k, shift - 1], bsend_sem.at[2 + shift, k])

        summed = branch[...]
        squares = add_over_rows(2 * layer + 1, jnp.sum(summed * summed, axis=1, keepdims=True))
        scale = lax.rsqrt(squares / model_width + norm_eps)
        current = (vals[...] + summed * scale * (1.0 + post_ref[layer])).astype(jnp.bfloat16)
        vals[...] = current.astype(jnp.float32)
        out_ref[...] = current
        return carry

    lax.fori_loop(0, layers, layer_step, 0)

    def drain(g, carry):
        wait_bytes(wbuf.at[g], wsend_sem.at[g])
        return carry

    lax.fori_loop(0, total_units, drain, 0)


def fused(row_count, col_count, tokens, pre_gain, post_gain, gate_weight, up_weight, down_weight):
    planes = col_count // 4
    own_tokens, own_width = tokens.shape
    layers, rows, _ = gate_weight.shape
    block = down_weight.shape[1]
    chunks = block // LANES
    units = planes * chunks
    total_units = layers * units
    every = col_count * own_tokens
    kpad = -(-2 * rows // LANES) * LANES
    piece = max(w for w in (128, 256, 384) if own_width % w == 0)
    steps = own_width // piece
    half = every // 2
    quarter = half // 2
    slots = 4
    bf16, f32 = jnp.bfloat16, jnp.float32
    dma = pltpu.SemaphoreType.DMA
    vmem = pl.BlockSpec(memory_space=pltpu.VMEM)
    hbm = pl.BlockSpec(memory_space=pl.ANY)
    scratch = [
        pltpu.VMEM((own_tokens, own_width), f32),
        pltpu.VMEM((2 * layers, own_tokens, LANES), f32),
        pltpu.VMEM((2 * layers, own_tokens, LANES), f32),
        pltpu.VMEM((own_width // (2 * rows), own_tokens, kpad), bf16),
        pltpu.VMEM((3, every, kpad), bf16),
        pltpu.VMEM((2, every, 2 * kpad), bf16),
        pltpu.VMEM((2, 2 * kpad, 4 * LANES), bf16),
        pltpu.VMEM((LAG + 1, every, 2 * LANES), f32),
        pltpu.VMEM((slots, every, 2 * LANES), bf16),
        pltpu.VMEM((units, every, 2 * LANES), bf16),
        pltpu.VMEM((slots, every, 2 * LANES), bf16),
        pltpu.VMEM(((planes - 1) * chunks, every, 2 * LANES), bf16),
        pltpu.VMEM((every, block), bf16),
        pltpu.VMEM((2, block, 2 * piece), bf16),
        pltpu.VMEM((steps, half, 2 * piece), bf16),
        pltpu.VMEM((steps, half, 2 * piece), bf16),
        pltpu.VMEM((steps, half, 2 * piece), f32),
        pltpu.VMEM((steps, half, piece), bf16),
        pltpu.VMEM((steps, half, piece), bf16),
        pltpu.VMEM((steps, quarter, piece), bf16),
        pltpu.VMEM((steps, quarter, piece), bf16),
        pltpu.VMEM((steps, quarter, piece), bf16),
        pltpu.VMEM((steps, planes - 1, own_tokens, piece), bf16),
        pltpu.VMEM((own_tokens, own_width), f32),
        dma((2 * layers,)),
        dma((2 * layers,)),
        dma((3,)),
        dma((3,)),
        dma((total_units,)),
        dma((total_units,)),
        dma((2,)),
        dma((slots,)),
        dma((units,)),
        dma((slots,)),
        dma(((planes - 1) * chunks,)),
        dma((2,)),
        dma((2 + planes, steps)),
        dma((2 + planes, steps)),
    ]
    out, _ = pl.pallas_call(
        functools.partial(fused_kernel, (layers, planes, chunks, steps)),
        out_shape=(
            jax.ShapeDtypeStruct(tokens.shape, bf16),
            jax.ShapeDtypeStruct((total_units, 3, rows, 4 * LANES), bf16),
        ),
        in_specs=[vmem, vmem, vmem, hbm, hbm, hbm],
        out_specs=(vmem, hbm),
        scratch_shapes=scratch,
        compiler_params=pltpu.CompilerParams(
            collective_id=0, has_side_effects=True, vmem_limit_bytes=64 * 1024 * 1024
        ),
        name="blocks",
    )(tokens, pre_gain[:, None, :], post_gain[:, None, :], gate_weight, up_weight, down_weight)
    return out


def activate(gate, up_proj):
    return (jax.nn.gelu(gate, approximate=True) * up_proj).astype(jnp.bfloat16)


def make_on_device(row_count, col_count):
    planes = 4 if col_count % 4 == 0 else 1
    inner = col_count // planes
    members = row_count * inner

    def swap(array, row_bits, plane_bits, seat_bits):
        pairs = []
        for row in range(row_count):
            for plane in range(planes):
                for seat in range(inner):
                    source = row * col_count + plane * inner + seat
                    target = (
                        (row ^ row_bits) * col_count
                        + (plane ^ plane_bits) * inner
                        + (seat ^ seat_bits)
                    )
                    pairs.append((source, target))
        return lax.ppermute(array, AXES, pairs)

    def sum_over_rows(array):
        total = array
        for bits in range(1, row_count):
            total = total + swap(array, bits, 0, 0)
        return total

    def on_device(tokens, pre_gain, post_gain, gate_weight, up_weight, down_weight):
        layer_count = gate_weight.shape[0]
        own_tokens, own_width = tokens.shape
        model_width = own_width * row_count
        stored_rows = gate_weight.shape[1]
        block_width = gate_weight.shape[2] // (row_count * col_count)
        plane_width = own_width // planes
        row = lax.axis_index("row")
        col = lax.axis_index("col")
        plane = col // inner
        seat = col % inner
        member = row * inner + seat

        def weight_chunk(layer_index, plane_bits, after):
            chunk_plane = plane ^ plane_bits
            if after is not None:
                chunk_plane, _ = lax.optimization_barrier((chunk_plane, after))
            held = jnp.zeros((members, stored_rows, 2 * block_width), jnp.bfloat16)
            for bits in range(members):
                row_bits, seat_bits = bits // inner, bits % inner
                start = (
                    (row ^ row_bits) * col_count + chunk_plane * inner + (seat ^ seat_bits)
                ) * block_width
                gate_part, up_part = (
                    lax.dynamic_slice(
                        weight, (layer_index, 0, start), (1, stored_rows, block_width)
                    )
                    for weight in (gate_weight, up_weight)
                )
                block = jnp.concatenate((gate_part, up_part), axis=2)
                if bits:
                    block = swap(block, row_bits, 0, seat_bits)
                held = lax.dynamic_update_slice(held, block, (member ^ bits, 0, 0))
            return held.reshape(members * stored_rows, 2 * block_width)

        def gather_plane(normed):
            parts = normed.reshape(own_tokens, planes, plane_width).transpose(1, 0, 2)
            held = jnp.zeros((planes, own_tokens, plane_width), jnp.bfloat16)
            for bits in range(planes):
                part = lax.dynamic_slice(
                    parts, (plane ^ bits, 0, 0), (1, own_tokens, plane_width)
                )
                if bits:
                    part = swap(part, 0, bits, 0)
                held = lax.dynamic_update_slice(held, part, (plane ^ bits, 0, 0))
            pieces = [held]
            for bits in range(1, row_count):
                pieces.append(swap(held, bits, 0, 0))
            rows = jnp.zeros((row_count,) + held.shape, jnp.bfloat16)
            for bits in range(row_count):
                rows = lax.dynamic_update_slice(rows, pieces[bits][None], (row ^ bits, 0, 0, 0))
            whole = rows.transpose(1, 2, 0, 3).reshape(
                planes, 1, own_tokens, row_count * plane_width
            )
            bit = inner // 2
            order = [0]
            blocks = whole
            while bit:
                blocks = jnp.concatenate((blocks, swap(blocks, 0, 0, bit)), axis=1)
                order = order + [seat_bits ^ bit for seat_bits in order]
                bit //= 2
            return blocks.reshape(planes * inner * own_tokens, row_count * plane_width), order

        def scatter_branch(branch):
            bit = 1
            halved_rows = False
            while bit < inner or not halved_rows:
                if bit < inner:
                    half = branch.shape[1] // 2
                    away = branch[:, half:].astype(jnp.bfloat16)
                    branch = branch[:, :half] + swap(away, 0, 0, bit).astype(jnp.float32)
                    bit *= 2
                if not halved_rows:
                    split = [
                        branch[..., i * own_width : (i + 1) * own_width]
                        for i in range(row_count)
                    ]

                    def part_of(wanted):
                        chosen = split[0]
                        for i in range(1, row_count):
                            chosen = jnp.where(wanted == i, split[i], chosen)
                        return chosen

                    total = part_of(row)
                    for bits in range(1, row_count):
                        away = part_of(row ^ bits).astype(jnp.bfloat16)
                        total = total + swap(away, bits, 0, 0).astype(jnp.float32)
                    branch = total
                    halved_rows = True
            branch = branch.reshape(planes, own_tokens, own_width)
            total = lax.dynamic_slice(branch, (plane, 0, 0), (1, own_tokens, own_width))
            for bits in range(1, planes):
                away = lax.dynamic_slice(
                    branch, (plane ^ bits, 0, 0), (1, own_tokens, own_width)
                ).astype(jnp.bfloat16)
                total = total + swap(away, 0, bits, 0).astype(jnp.float32)
            return total[0]

        current = tokens
        landed = []
        for layer_index in range(layer_count):
            values = current.astype(jnp.float32)
            squares = sum_over_rows(jnp.sum(values * values, axis=1, keepdims=True))
            scale_pre = lax.rsqrt(squares / model_width + norm_eps)
            normed = (values * scale_pre * (1.0 + pre_gain[layer_index])[None, :]).astype(
                jnp.bfloat16
            )
            gathered, order = gather_plane(normed)
            arrived = []
            for bits in reversed(range(planes)):
                after = landed[-2] if len(landed) > 1 else gathered if landed else None
                chunk = weight_chunk(layer_index, bits, after)
                landed.append(chunk)
                part = jnp.dot(gathered, chunk, preferred_element_type=jnp.float32)
                if bits:
                    part = swap(part.astype(jnp.bfloat16), 0, bits, 0)
                arrived.append(part)
            summed = arrived[-1]
            for part in arrived[:-1]:
                summed = summed + part.astype(jnp.float32)
            hidden = activate(summed[:, :block_width], summed[:, block_width:])
            branch = jnp.dot(hidden, down_weight[layer_index], preferred_element_type=jnp.float32)
            branch = branch.reshape(planes, inner, own_tokens, model_width)
            branch = scatter_branch(branch)
            branch_squares = sum_over_rows(jnp.sum(branch * branch, axis=1, keepdims=True))
            scale_post = lax.rsqrt(branch_squares / model_width + norm_eps)
            post = branch * scale_post * (1.0 + post_gain[layer_index])[None, :]
            current = (values + post).astype(jnp.bfloat16)
        return current

    return on_device


def solution(mesh):
    in_specs = (
        P("col", "row"),
        P(None, "row"),
        P(None, "row"),
        P(None, ("row", "col"), None),
        P(None, ("row", "col"), None),
        P(None, ("row", "col"), None),
    )
    out_specs = P("col", "row")
    sizes = mesh.shape["row"], mesh.shape["col"]
    permuted = make_on_device(*sizes)

    def on_device(*arrays):
        tokens, _, _, gate_weight, _, down_weight = arrays
        if fits(*sizes, (tokens.shape, gate_weight.shape, down_weight.shape)):
            return fused(*sizes, *arrays)
        return permuted(*arrays)

    return jax.shard_map(
        on_device, mesh=mesh, in_specs=in_specs, out_specs=out_specs, check_vma=False
    )
```

```python
import functools

import jax
import jax.numpy as jnp
from jax import lax
from jax.experimental import pallas as pl
from jax.experimental.pallas import tpu as pltpu
from jax.sharding import PartitionSpec as P

norm_eps = 1e-06
AXES = ("row", "col")
MESH = pl.DeviceIdType.MESH
LANES = 128

AHEAD = 6
EXTRA = 0
LAG = 3


def div(a, b):
    return lax.div(a, jnp.int32(b))


def rem(a, b):
    return lax.rem(a, jnp.int32(b))


def fits(row_count, col_count, shapes):
    (_, width), (_, rows, hidden), (_, block, _) = shapes
    return (
        row_count == 2
        and col_count % 4 == 0
        and rows % 16 == 0
        and block % LANES == 0
        and width % LANES == 0
    )


def fused_kernel(
    dims,
    tokens_ref,
    pre_ref,
    post_ref,
    gate_ref,
    up_ref,
    down_ref,
    out_ref,
    wbuf,
    vals,
    ssend,
    srecv,
    nstage,
    nrecv,
    lhs,
    tile,
    acc,
    ysend,
    yrecv,
    zsend,
    zrecv,
    hidden,
    dtile,
    csend,
    crecv,
    bacc,
    xs,
    xr,
    ys,
    yr,
    qs,
    qr,
    zs,
    zr,
    branch,
    ssend_sem,
    srecv_sem,
    nsend_sem,
    nrecv_sem,
    wsend_sem,
    wrecv_sem,
    tile_sem,
    ysend_sem,
    yrecv_sem,
    zsend_sem,
    zrecv_sem,
    dtile_sem,
    bsend_sem,
    brecv_sem,
):
    layers, planes, chunks, steps = dims
    cols = planes * 4
    own_tokens, own_width = tokens_ref.shape
    model_width = 2 * own_width
    rows = gate_ref.shape[1]
    block = down_ref.shape[1]
    kpad = nstage.shape[2]
    units = planes * chunks
    total_units = layers * units
    slots = ysend.shape[0]
    acc_slots = acc.shape[0]
    half = cols // 2 * own_tokens
    quarter = half // 2
    piece = xs.shape[2]

    x = lax.axis_index("row")
    col = lax.axis_index("col")
    z, y, c = div(col, 4), rem(div(col, 2), 2), rem(col, 2)

    def place(px, pz, py, pc):
        return (px, pz * 4 + py * 2 + pc)

    def send(src, dst, send_sem, recv_sem, to):
        copy = pltpu.make_async_remote_copy(
            src_ref=src,
            dst_ref=dst,
            send_sem=send_sem,
            recv_sem=recv_sem,
            device_id=to,
            device_id_type=MESH,
        )
        copy.start()

    def wait_bytes(ref, sem):
        pltpu.make_async_copy(ref, ref, sem).wait()

    def offset(value, size):
        return pl.multiple_of(value, size)

    barrier = pltpu.get_barrier_semaphore()

    def greet(i, carry):
        other = rem(x * cols + col + i, 2 * cols)
        pl.semaphore_signal(
            barrier, inc=1, device_id=(div(other, cols), rem(other, cols)), device_id_type=MESH
        )
        return carry

    lax.fori_loop(1, 2 * cols, greet, 0)
    pl.semaphore_wait(barrier, 2 * cols - 1)

    def unit_of(u):
        later = div(u + units - (planes - 1), units)
        last = div(u + 1, units)
        r = (1 - later) * u + later * rem(u + 1, planes)
        shift = (planes - 1 - r) * (1 - last)
        own = 1 - div(shift + planes - 1, planes)
        return shift, div(u + 1, planes) - own, rem(u, 2)

    def issue_weights(g):
        layer = div(g, units)
        shift, j, s = unit_of(rem(g, units))
        pz = rem(z + shift, planes)
        for da, dc in ((0, 1), (1, 0), (1, 1)):
            px = rem(x + da * (1 - s), 2)
            py = rem(y + da * s, 2)
            pc = rem(c + dc, 2)
            slot = 2 * da + dc - 1
            for db in range(2):
                ox = rem(px + db * s, 2)
                oy = rem(py + db * (1 - s), 2)
                owner = ox * cols + pz * 4 + oy * 2 + pc
                start = offset(owner * block + j * LANES, LANES)
                for which, ref in enumerate((gate_ref, up_ref)):
                    send(
                        ref.at[layer, :, pl.ds(start, LANES)],
                        wbuf.at[g, slot, :, pl.ds((2 * db + which) * LANES, LANES)],
                        wsend_sem.at[g],
                        wrecv_sem.at[g],
                        place(px, z, py, pc),
                    )

    def issue_if(g):
        @pl.when(g < total_units)
        def _():
            issue_weights(g)

    def load_tile(g, slot):
        layer = div(g, units)
        shift, j, s = unit_of(rem(g, units))
        pz = rem(z + shift, planes)
        for db in range(2):
            ox = rem(x + db * s, 2)
            oy = rem(y + db * (1 - s), 2)
            owner = ox * cols + pz * 4 + oy * 2 + c
            start = offset(owner * block + j * LANES, LANES)
            for which, ref in enumerate((gate_ref, up_ref)):
                pltpu.make_async_copy(
                    ref.at[layer, :, pl.ds(start, LANES)],
                    tile.at[
                        slot,
                        pl.ds(offset(c * rows, 16), rows),
                        pl.ds((2 * db + which) * LANES, LANES),
                    ],
                    tile_sem.at[slot],
                ).start()
        for da, dc in ((0, 1), (1, 0), (1, 1)):
            pc = rem(c + dc, 2)
            pltpu.make_async_copy(
                wbuf.at[g, 2 * da + dc - 1],
                tile.at[slot, pl.ds(offset(da * kpad + pc * rows, 16), rows), :],
                tile_sem.at[slot],
            ).start()

    def wait_tile(slot):
        wait_bytes(tile.at[slot, pl.ds(0, 4 * rows), :], tile_sem.at[slot])

    def load_down(layer, k, slot):
        for i in range(2):
            px = rem(x + i, 2)
            pltpu.make_async_copy(
                down_ref.at[layer, :, pl.ds(offset(px * own_width + k * piece, LANES), piece)],
                dtile.at[slot, :, pl.ds(i * piece, piece)],
                dtile_sem.at[slot],
            ).start()

    def add_over_rows(index, squares):
        ssend[index] = jnp.broadcast_to(squares, ssend.shape[1:])
        send(
            ssend.at[index], srecv.at[index], ssend_sem.at[index], srecv_sem.at[index], (1 - x, col)
        )
        wait_bytes(srecv.at[index], srecv_sem.at[index])
        wait_bytes(ssend.at[index], ssend_sem.at[index])
        return squares + srecv[index][:, 0:1]

    for g in range(AHEAD):
        issue_weights(jnp.int32(g))

    nstage[...] = jnp.zeros_like(nstage)
    tile[...] = jnp.zeros_like(tile)
    vals[...] = tokens_ref[...].astype(jnp.float32)

    def layer_step(layer, carry):
        load_down(layer, 0, 0)
        load_down(layer, 1, 1)
        values = vals[...]
        squares = add_over_rows(2 * layer, jnp.sum(values * values, axis=1, keepdims=True))
        scale = lax.rsqrt(squares / model_width + norm_eps)
        normed = values * scale * (1.0 + pre_ref[layer])
        width = 2 * rows
        for q in range(own_width // width):
            nstage[q, :, 0:width] = normed[:, q * width : (q + 1) * width].astype(jnp.bfloat16)

        here = offset((c * (cols // 2) + y * planes + z) * own_tokens, own_tokens)
        lines = pl.ds(here, own_tokens)

        half_here = pl.ds(offset(c * half, half), half)

        def scatter(i, carry):
            other = rem(2 * z + y + i, cols // 2)
            send(
                nstage.at[other],
                nrecv.at[0, lines, :],
                nsend_sem.at[0],
                nrecv_sem.at[0],
                (x, other * 2 + c),
            )
            return carry

        lax.fori_loop(1, cols // 2, scatter, 0)
        nrecv[0, lines, :] = nstage[z * 2 + y]
        most = nrecv.at[0, pl.ds(0, half - own_tokens), :]
        wait_bytes(most, nrecv_sem.at[0])
        part = nrecv.at[0, half_here, :]
        for slot, to in enumerate(
            (place(x, z, y, 1 - c), place(1 - x, z, y, c), place(x, z, 1 - y, c))
        ):
            send(
                part,
                nrecv.at[slot, half_here, :],
                nsend_sem.at[1 + slot],
                nrecv_sem.at[1 + slot],
                to,
            )
        for slot in (1, 2):
            wait_bytes(part, nrecv_sem.at[1 + slot])
            send(
                nrecv.at[slot, half_here, :],
                nrecv.at[slot, half_here, :],
                nsend_sem.at[3 + slot],
                nrecv_sem.at[3 + slot],
                place(x, z, y, 1 - c),
            )
        for i in (1, 4, 5):
            wait_bytes(part, nrecv_sem.at[i])
        wait_bytes(most, nsend_sem.at[0])
        for i in range(1, 6):
            wait_bytes(part, nsend_sem.at[i])
        for s in range(2):
            lhs[s, :, 0:kpad] = nrecv[0]
            lhs[s, :, kpad : 2 * kpad] = nrecv[1 + s]

        def unit_step(u, carry):
            g = layer * units + u
            slot = rem(u, 2)

            @pl.when(u < units)
            def _():
                issue_if(g + AHEAD + EXTRA * layer)
                wait_bytes(wbuf.at[g], wrecv_sem.at[g])
                load_tile(g, slot)

            v = u - LAG

            @pl.when(v >= 0)
            def _():
                shift, j, s = unit_of(v)
                wait_bytes(yrecv.at[v], yrecv_sem.at[v])
                summed = acc[rem(v, acc_slots)] + yrecv[v].astype(jnp.float32)

                @pl.when(shift > 0)
                def _():
                    sent = j * (planes - 1) + planes - 1 - shift
                    out = rem(sent, slots)

                    @pl.when(sent >= slots)
                    def _():
                        wait_bytes(zsend.at[out], zsend_sem.at[out])

                    zsend[out] = summed.astype(jnp.bfloat16)
                    at = (shift - 1) * chunks + j
                    send(
                        zsend.at[out],
                        zrecv.at[at],
                        zsend_sem.at[out],
                        zrecv_sem.at[at],
                        place(x, rem(z + shift, planes), y, c),
                    )

                @pl.when(shift == 0)
                def _():
                    whole = summed
                    for i in range(planes - 1):
                        at = i * chunks + j
                        wait_bytes(zrecv.at[at], zrecv_sem.at[at])
                        whole = whole + zrecv[at].astype(jnp.float32)
                    gate, up_proj = whole[:, :LANES], whole[:, LANES:]
                    hidden[:, pl.ds(offset(j * LANES, LANES), LANES)] = (
                        jax.nn.gelu(gate, approximate=True) * up_proj
                    ).astype(jnp.bfloat16)

            @pl.when(u < units)
            def _():
                shift, j, s = unit_of(u)
                wait_tile(slot)
                part = jnp.dot(lhs[s], tile[slot], preferred_element_type=jnp.float32)
                out = rem(u, slots)

                @pl.when(u >= slots)
                def _():
                    wait_bytes(ysend.at[out], ysend_sem.at[out])

                ysend[out] = part[:, 2 * LANES :].astype(jnp.bfloat16)
                acc[rem(u, acc_slots)] = part[:, : 2 * LANES]
                send(
                    ysend.at[out],
                    yrecv.at[u],
                    ysend_sem.at[out],
                    yrecv_sem.at[u],
                    place(rem(x + s, 2), z, rem(y + 1 - s, 2), c),
                )

            return carry

        lax.fori_loop(0, units + LAG, unit_step, 0)
        for out in range(min(slots, units)):
            wait_bytes(ysend.at[out], ysend_sem.at[out])
        for out in range(min(slots, units - chunks)):
            wait_bytes(zsend.at[out], zsend_sem.at[out])

        own_half = pl.ds(offset(c * half, half), half)
        far_half = pl.ds(offset((1 - c) * half, half), half)
        own_quarter = pl.ds(offset(y * quarter, quarter), quarter)
        far_quarter = pl.ds(offset((1 - y) * quarter, quarter), quarter)
        own_lines = pl.ds(offset(z * own_tokens, own_tokens), own_tokens)

        def multiply(k):
            slot = k % 2
            wait_bytes(dtile.at[slot], dtile_sem.at[slot])
            csend[k] = jnp.dot(
                hidden[far_half, :], dtile[slot], preferred_element_type=jnp.float32
            ).astype(jnp.bfloat16)
            send(
                csend.at[k], crecv.at[k], bsend_sem.at[0, k], brecv_sem.at[0, k], place(x, z, y, 1 - c)
            )
            bacc[k] = jnp.dot(hidden[own_half, :], dtile[slot], preferred_element_type=jnp.float32)
            if k + 2 < steps:
                load_down(layer, k + 2, slot)

        to_x, to_y = place(1 - x, z, y, c), place(x, z, 1 - y, c)

        def over_first(k):
            wait_bytes(crecv.at[k], brecv_sem.at[0, k])
            summed = bacc[k] + crecv[k].astype(jnp.float32)
            i = k // 2
            if k % 2 == 0:
                bacc[k, :, 0:piece] = summed[:, :piece]
                xs[i] = summed[:, piece:].astype(jnp.bfloat16)
                send(xs.at[i], xr.at[i], bsend_sem.at[1, k], brecv_sem.at[1, k], to_x)
            else:
                bacc[k] = summed
                ys[i] = bacc[k, far_quarter, :].astype(jnp.bfloat16)
                send(ys.at[i], yr.at[i], bsend_sem.at[1, k], brecv_sem.at[1, k], to_y)

        def over_second(k):
            i = k // 2
            if k % 2 == 0:
                wait_bytes(xr.at[i], brecv_sem.at[1, k])
                bacc[k, :, 0:piece] = bacc[k, :, 0:piece] + xr[i].astype(jnp.float32)
                qs[k] = bacc[k, far_quarter, 0:piece].astype(jnp.bfloat16)
                bacc[k, 0:quarter, 0:piece] = bacc[k, own_quarter, 0:piece]
                send(qs.at[k], qr.at[k], bsend_sem.at[2, k], brecv_sem.at[2, k], to_y)
            else:
                wait_bytes(yr.at[i], brecv_sem.at[1, k])
                summed = bacc[k, own_quarter, :] + yr[i].astype(jnp.float32)
                qs[k] = summed[:, piece:].astype(jnp.bfloat16)
                bacc[k, 0:quarter, 0:piece] = summed[:, :piece]
                send(qs.at[k], qr.at[k], bsend_sem.at[2, k], brecv_sem.at[2, k], to_x)

        def over_z(k):
            wait_bytes(qr.at[k], brecv_sem.at[2, k])
            summed = bacc[k, 0:quarter, 0:piece] + qr[k].astype(jnp.float32)
            bacc[k, 0:quarter, 0:piece] = summed
            zs[k] = summed.astype(jnp.bfloat16)
            for shift in range(1, planes):
                pz = rem(z + shift, planes)
                send(
                    zs.at[k, pl.ds(offset(pz * own_tokens, own_tokens), own_tokens), :],
                    zr.at[k, shift - 1],
                    bsend_sem.at[2 + shift, k],
                    brecv_sem.at[2 + shift, k],
                    place(x, pz, y, c),
                )

        def finish(k):
            total = bacc[k, own_lines, 0:piece]
            for shift in range(1, planes):
                wait_bytes(zr.at[k, shift - 1], brecv_sem.at[2 + shift, k])
                total = total + zr[k, shift - 1].astype(jnp.float32)
            branch[:, k * piece : (k + 1) * piece] = total

        stages = (multiply, over_first, over_second, over_z, finish)
        for t in range(steps + len(stages) - 1):
            for lag, stage in enumerate(stages):
                if 0 <= t - lag < steps:
                    stage(t - lag)
            if t < EXTRA:
                issue_if((layer + 1) * units + AHEAD + EXTRA * layer + t)
        for t in range(steps + len(stages) - 1, EXTRA):
            issue_if((layer + 1) * units + AHEAD + EXTRA * layer + t)
        for k in range(steps):
            wait_bytes(csend.at[k], bsend_sem.at[0, k])
            wait_bytes((xs, ys)[k % 2].at[k // 2], bsend_sem.at[1, k])
            wait_bytes(qs.at[k], bsend_sem.at[2, k])
            for shift in range(1, planes):
                wait_bytes(zr.at[k, shift - 1], bsend_sem.at[2 + shift, k])

        summed = branch[...]
        squares = add_over_rows(2 * layer + 1, jnp.sum(summed * summed, axis=1, keepdims=True))
        scale = lax.rsqrt(squares / model_width + norm_eps)
        current = (vals[...] + summed * scale * (1.0 + post_ref[layer])).astype(jnp.bfloat16)
        vals[...] = current.astype(jnp.float32)
        out_ref[...] = current
        return carry

    lax.fori_loop(0, layers, layer_step, 0)

    def drain(g, carry):
        wait_bytes(wbuf.at[g], wsend_sem.at[g])
        return carry

    lax.fori_loop(0, total_units, drain, 0)


def fused(row_count, col_count, tokens, pre_gain, post_gain, gate_weight, up_weight, down_weight):
    planes = col_count // 4
    own_tokens, own_width = tokens.shape
    layers, rows, _ = gate_weight.shape
    block = down_weight.shape[1]
    chunks = block // LANES
    units = planes * chunks
    total_units = layers * units
    every = col_count * own_tokens
    kpad = -(-2 * rows // LANES) * LANES
    piece = max(w for w in (128, 256, 384) if own_width % w == 0)
    steps = own_width // piece
    half = every // 2
    quarter = half // 2
    slots = 4
    bf16, f32 = jnp.bfloat16, jnp.float32
    dma = pltpu.SemaphoreType.DMA
    vmem = pl.BlockSpec(memory_space=pltpu.VMEM)
    hbm = pl.BlockSpec(memory_space=pl.ANY)
    scratch = [
        pltpu.VMEM((own_tokens, own_width), f32),
        pltpu.VMEM((2 * layers, own_tokens, LANES), f32),
        pltpu.VMEM((2 * layers, own_tokens, LANES), f32),
        pltpu.VMEM((own_width // (2 * rows), own_tokens, kpad), bf16),
        pltpu.VMEM((3, every, kpad), bf16),
        pltpu.VMEM((2, every, 2 * kpad), bf16),
        pltpu.VMEM((2, 2 * kpad, 4 * LANES), bf16),
        pltpu.VMEM((LAG + 1, every, 2 * LANES), f32),
        pltpu.VMEM((slots, every, 2 * LANES), bf16),
        pltpu.VMEM((units, every, 2 * LANES), bf16),
        pltpu.VMEM((slots, every, 2 * LANES), bf16),
        pltpu.VMEM(((planes - 1) * chunks, every, 2 * LANES), bf16),
        pltpu.VMEM((every, block), bf16),
        pltpu.VMEM((2, block, 2 * piece), bf16),
        pltpu.VMEM((steps, half, 2 * piece), bf16),
        pltpu.VMEM((steps, half, 2 * piece), bf16),
        pltpu.VMEM((steps, half, 2 * piece), f32),
        pltpu.VMEM((-(-steps // 2), half, piece), bf16),
        pltpu.VMEM((-(-steps // 2), half, piece), bf16),
        pltpu.VMEM((-(-steps // 2), quarter, 2 * piece), bf16),
        pltpu.VMEM((-(-steps // 2), quarter, 2 * piece), bf16),
        pltpu.VMEM((steps, quarter, piece), bf16),
        pltpu.VMEM((steps, quarter, piece), bf16),
        pltpu.VMEM((steps, quarter, piece), bf16),
        pltpu.VMEM((steps, planes - 1, own_tokens, piece), bf16),
        pltpu.VMEM((own_tokens, own_width), f32),
        dma((2 * layers,)),
        dma((2 * layers,)),
        dma((6,)),
        dma((6,)),
        dma((total_units,)),
        dma((total_units,)),
        dma((2,)),
        dma((slots,)),
        dma((units,)),
        dma((slots,)),
        dma(((planes - 1) * chunks,)),
        dma((2,)),
        dma((2 + planes, steps)),
        dma((2 + planes, steps)),
    ]
    out, _ = pl.pallas_call(
        functools.partial(fused_kernel, (layers, planes, chunks, steps)),
        out_shape=(
            jax.ShapeDtypeStruct(tokens.shape, bf16),
            jax.ShapeDtypeStruct((total_units, 3, rows, 4 * LANES), bf16),
        ),
        in_specs=[vmem, vmem, vmem, hbm, hbm, hbm],
        out_specs=(vmem, hbm),
        scratch_shapes=scratch,
        compiler_params=pltpu.CompilerParams(
            collective_id=0, has_side_effects=True, vmem_limit_bytes=64 * 1024 * 1024
        ),
        name="blocks",
    )(tokens, pre_gain[:, None, :], post_gain[:, None, :], gate_weight, up_weight, down_weight)
    return out


def activate(gate, up_proj):
    return (jax.nn.gelu(gate, approximate=True) * up_proj).astype(jnp.bfloat16)


def make_on_device(row_count, col_count):
    planes = 4 if col_count % 4 == 0 else 1
    inner = col_count // planes
    members = row_count * inner

    def swap(array, row_bits, plane_bits, seat_bits):
        pairs = []
        for row in range(row_count):
            for plane in range(planes):
                for seat in range(inner):
                    source = row * col_count + plane * inner + seat
                    target = (
                        (row ^ row_bits) * col_count
                        + (plane ^ plane_bits) * inner
                        + (seat ^ seat_bits)
                    )
                    pairs.append((source, target))
        return lax.ppermute(array, AXES, pairs)

    def sum_over_rows(array):
        total = array
        for bits in range(1, row_count):
            total = total + swap(array, bits, 0, 0)
        return total

    def on_device(tokens, pre_gain, post_gain, gate_weight, up_weight, down_weight):
        layer_count = gate_weight.shape[0]
        own_tokens, own_width = tokens.shape
        model_width = own_width * row_count
        stored_rows = gate_weight.shape[1]
        block_width = gate_weight.shape[2] // (row_count * col_count)
        plane_width = own_width // planes
        row = lax.axis_index("row")
        col = lax.axis_index("col")
        plane = col // inner
        seat = col % inner
        member = row * inner + seat

        def weight_chunk(layer_index, plane_bits, after):
            chunk_plane = plane ^ plane_bits
            if after is not None:
                chunk_plane, _ = lax.optimization_barrier((chunk_plane, after))
            held = jnp.zeros((members, stored_rows, 2 * block_width), jnp.bfloat16)
            for bits in range(members):
                row_bits, seat_bits = bits // inner, bits % inner
                start = (
                    (row ^ row_bits) * col_count + chunk_plane * inner + (seat ^ seat_bits)
                ) * block_width
                gate_part, up_part = (
                    lax.dynamic_slice(
                        weight, (layer_index, 0, start), (1, stored_rows, block_width)
                    )
                    for weight in (gate_weight, up_weight)
                )
                block = jnp.concatenate((gate_part, up_part), axis=2)
                if bits:
                    block = swap(block, row_bits, 0, seat_bits)
                held = lax.dynamic_update_slice(held, block, (member ^ bits, 0, 0))
            return held.reshape(members * stored_rows, 2 * block_width)

        def gather_plane(normed):
            parts = normed.reshape(own_tokens, planes, plane_width).transpose(1, 0, 2)
            held = jnp.zeros((planes, own_tokens, plane_width), jnp.bfloat16)
            for bits in range(planes):
                part = lax.dynamic_slice(
                    parts, (plane ^ bits, 0, 0), (1, own_tokens, plane_width)
                )
                if bits:
                    part = swap(part, 0, bits, 0)
                held = lax.dynamic_update_slice(held, part, (plane ^ bits, 0, 0))
            pieces = [held]
            for bits in range(1, row_count):
                pieces.append(swap(held, bits, 0, 0))
            rows = jnp.zeros((row_count,) + held.shape, jnp.bfloat16)
            for bits in range(row_count):
                rows = lax.dynamic_update_slice(rows, pieces[bits][None], (row ^ bits, 0, 0, 0))
            whole = rows.transpose(1, 2, 0, 3).reshape(
                planes, 1, own_tokens, row_count * plane_width
            )
            bit = inner // 2
            order = [0]
            blocks = whole
            while bit:
                blocks = jnp.concatenate((blocks, swap(blocks, 0, 0, bit)), axis=1)
                order = order + [seat_bits ^ bit for seat_bits in order]
                bit //= 2
            return blocks.reshape(planes * inner * own_tokens, row_count * plane_width), order

        def scatter_branch(branch):
            bit = 1
            halved_rows = False
            while bit < inner or not halved_rows:
                if bit < inner:
                    half = branch.shape[1] // 2
                    away = branch[:, half:].astype(jnp.bfloat16)
                    branch = branch[:, :half] + swap(away, 0, 0, bit).astype(jnp.float32)
                    bit *= 2
                if not halved_rows:
                    split = [
                        branch[..., i * own_width : (i + 1) * own_width]
                        for i in range(row_count)
                    ]

                    def part_of(wanted):
                        chosen = split[0]
                        for i in range(1, row_count):
                            chosen = jnp.where(wanted == i, split[i], chosen)
                        return chosen

                    total = part_of(row)
                    for bits in range(1, row_count):
                        away = part_of(row ^ bits).astype(jnp.bfloat16)
                        total = total + swap(away, bits, 0, 0).astype(jnp.float32)
                    branch = total
                    halved_rows = True
            branch = branch.reshape(planes, own_tokens, own_width)
            total = lax.dynamic_slice(branch, (plane, 0, 0), (1, own_tokens, own_width))
            for bits in range(1, planes):
                away = lax.dynamic_slice(
                    branch, (plane ^ bits, 0, 0), (1, own_tokens, own_width)
                ).astype(jnp.bfloat16)
                total = total + swap(away, 0, bits, 0).astype(jnp.float32)
            return total[0]

        current = tokens
        landed = []
        for layer_index in range(layer_count):
            values = current.astype(jnp.float32)
            squares = sum_over_rows(jnp.sum(values * values, axis=1, keepdims=True))
            scale_pre = lax.rsqrt(squares / model_width + norm_eps)
            normed = (values * scale_pre * (1.0 + pre_gain[layer_index])[None, :]).astype(
                jnp.bfloat16
            )
            gathered, order = gather_plane(normed)
            arrived = []
            for bits in reversed(range(planes)):
                after = landed[-2] if len(landed) > 1 else gathered if landed else None
                chunk = weight_chunk(layer_index, bits, after)
                landed.append(chunk)
                part = jnp.dot(gathered, chunk, preferred_element_type=jnp.float32)
                if bits:
                    part = swap(part.astype(jnp.bfloat16), 0, bits, 0)
                arrived.append(part)
            summed = arrived[-1]
            for part in arrived[:-1]:
                summed = summed + part.astype(jnp.float32)
            hidden = activate(summed[:, :block_width], summed[:, block_width:])
            branch = jnp.dot(hidden, down_weight[layer_index], preferred_element_type=jnp.float32)
            branch = branch.reshape(planes, inner, own_tokens, model_width)
            branch = scatter_branch(branch)
            branch_squares = sum_over_rows(jnp.sum(branch * branch, axis=1, keepdims=True))
            scale_post = lax.rsqrt(branch_squares / model_width + norm_eps)
            post = branch * scale_post * (1.0 + post_gain[layer_index])[None, :]
            current = (values + post).astype(jnp.bfloat16)
        return current

    return on_device


def solution(mesh):
    in_specs = (
        P("col", "row"),
        P(None, "row"),
        P(None, "row"),
        P(None, ("row", "col"), None),
        P(None, ("row", "col"), None),
        P(None, ("row", "col"), None),
    )
    out_specs = P("col", "row")
    sizes = mesh.shape["row"], mesh.shape["col"]
    permuted = make_on_device(*sizes)

    def on_device(*arrays):
        tokens, _, _, gate_weight, _, down_weight = arrays
        if fits(*sizes, (tokens.shape, gate_weight.shape, down_weight.shape)):
            return fused(*sizes, *arrays)
        return permuted(*arrays)

    return jax.shard_map(
        on_device, mesh=mesh, in_specs=in_specs, out_specs=out_specs, check_vma=False
    )
```

```python
import functools

import jax
import jax.numpy as jnp
from jax import lax
from jax.experimental import pallas as pl
from jax.experimental.pallas import tpu as pltpu
from jax.sharding import PartitionSpec as P

norm_eps = 1e-06
AXES = ("row", "col")
MESH = pl.DeviceIdType.MESH
LANES = 128

AHEAD = 6
EXTRA = 0
LAG = 3


def div(a, b):
    return lax.div(a, jnp.int32(b))


def rem(a, b):
    return lax.rem(a, jnp.int32(b))


def fits(row_count, col_count, shapes):
    (_, width), (_, rows, hidden), (_, block, _) = shapes
    return (
        row_count == 2
        and col_count == 16
        and rows % 16 == 0
        and block % LANES == 0
        and width % LANES == 0
    )


def fused_kernel(
    dims,
    tokens_ref,
    pre_ref,
    post_ref,
    gate_ref,
    up_ref,
    down_ref,
    out_ref,
    wbuf,
    vals,
    ssend,
    srecv,
    nstage,
    nrecv,
    lhs,
    tile,
    acc,
    ysend,
    yrecv,
    zsend,
    zrecv,
    hidden,
    dtile,
    csend,
    crecv,
    bacc,
    xs,
    xr,
    ys,
    yr,
    qs,
    qr,
    zs,
    zr,
    branch,
    ssend_sem,
    srecv_sem,
    nsend_sem,
    nrecv_sem,
    wsend_sem,
    wrecv_sem,
    tile_sem,
    ysend_sem,
    yrecv_sem,
    zsend_sem,
    zrecv_sem,
    dtile_sem,
    bsend_sem,
    brecv_sem,
):
    layers, planes, chunks, steps = dims
    cols = planes * 4
    own_tokens, own_width = tokens_ref.shape
    model_width = 2 * own_width
    rows = gate_ref.shape[1]
    block = down_ref.shape[1]
    kpad = nstage.shape[2]
    units = planes * chunks
    total_units = layers * units
    slots = ysend.shape[0]
    acc_slots = acc.shape[0]
    half = cols // 2 * own_tokens
    quarter = half // 2
    piece = xs.shape[2]

    x = lax.axis_index("row")
    col = lax.axis_index("col")
    z, y, c = div(col, 4), rem(div(col, 2), 2), rem(col, 2)

    def place(px, pz, py, pc):
        return (px, pz * 4 + py * 2 + pc)

    def send(src, dst, send_sem, recv_sem, to):
        copy = pltpu.make_async_remote_copy(
            src_ref=src,
            dst_ref=dst,
            send_sem=send_sem,
            recv_sem=recv_sem,
            device_id=to,
            device_id_type=MESH,
        )
        copy.start()

    def wait_bytes(ref, sem):
        pltpu.make_async_copy(ref, ref, sem).wait()

    def offset(value, size):
        return pl.multiple_of(value, size)

    barrier = pltpu.get_barrier_semaphore()

    def greet(i, carry):
        other = rem(x * cols + col + i, 2 * cols)
        pl.semaphore_signal(
            barrier, inc=1, device_id=(div(other, cols), rem(other, cols)), device_id_type=MESH
        )
        return carry

    lax.fori_loop(1, 2 * cols, greet, 0)
    pl.semaphore_wait(barrier, 2 * cols - 1)

    high = div(z, 2)
    inner = (1 - high) * z + high * (planes - 1 - z)

    def plane_of(d):
        return (1 - high) * d + high * (planes - 1 - d)

    def unit_of(u):
        later = div(u + units - (planes - 1), units)
        last = div(u + 1, units)
        r = later * rem(u + 1, planes)
        r_end = (1 - later) * u + r
        r_in = (1 - later) * (u + div(u + 1, 2)) + r
        d = (1 - inner) * (3 - r_end) + inner * (r_in + div(r_in, 2) - 2 * div(r_in, 3))
        d = (1 - last) * d + last * inner
        own = 1 - div((d - inner) * (d - inner) + 8, 9)
        return d, own, div(u + 1, planes) - own, rem(u, 2)

    def issue_weights(g):
        layer = div(g, units)
        d, _, j, s = unit_of(rem(g, units))
        pz = plane_of(d)
        for da, dc in ((0, 1), (1, 0), (1, 1)):
            px = rem(x + da * (1 - s), 2)
            py = rem(y + da * s, 2)
            pc = rem(c + dc, 2)
            slot = 2 * da + dc - 1
            for db in range(2):
                ox = rem(px + db * s, 2)
                oy = rem(py + db * (1 - s), 2)
                owner = ox * cols + pz * 4 + oy * 2 + pc
                start = offset(owner * block + j * LANES, LANES)
                for which, ref in enumerate((gate_ref, up_ref)):
                    send(
                        ref.at[layer, :, pl.ds(start, LANES)],
                        wbuf.at[g, slot, :, pl.ds((2 * db + which) * LANES, LANES)],
                        wsend_sem.at[g],
                        wrecv_sem.at[g],
                        place(px, z, py, pc),
                    )

    def issue_if(g):
        @pl.when(g < total_units)
        def _():
            issue_weights(g)

    def load_tile(g, slot):
        layer = div(g, units)
        d, _, j, s = unit_of(rem(g, units))
        pz = plane_of(d)
        for db in range(2):
            ox = rem(x + db * s, 2)
            oy = rem(y + db * (1 - s), 2)
            owner = ox * cols + pz * 4 + oy * 2 + c
            start = offset(owner * block + j * LANES, LANES)
            for which, ref in enumerate((gate_ref, up_ref)):
                pltpu.make_async_copy(
                    ref.at[layer, :, pl.ds(start, LANES)],
                    tile.at[
                        slot,
                        pl.ds(offset(c * rows, 16), rows),
                        pl.ds((2 * db + which) * LANES, LANES),
                    ],
                    tile_sem.at[slot],
                ).start()
        for da, dc in ((0, 1), (1, 0), (1, 1)):
            pc = rem(c + dc, 2)
            pltpu.make_async_copy(
                wbuf.at[g, 2 * da + dc - 1],
                tile.at[slot, pl.ds(offset(da * kpad + pc * rows, 16), rows), :],
                tile_sem.at[slot],
            ).start()

    def wait_tile(slot):
        wait_bytes(tile.at[slot, pl.ds(0, 4 * rows), :], tile_sem.at[slot])

    def load_down(layer, k, slot):
        for i in range(2):
            px = rem(x + i, 2)
            pltpu.make_async_copy(
                down_ref.at[layer, :, pl.ds(offset(px * own_width + k * piece, LANES), piece)],
                dtile.at[slot, :, pl.ds(i * piece, piece)],
                dtile_sem.at[slot],
            ).start()

    def add_over_rows(index, squares):
        ssend[index] = jnp.broadcast_to(squares, ssend.shape[1:])
        send(
            ssend.at[index], srecv.at[index], ssend_sem.at[index], srecv_sem.at[index], (1 - x, col)
        )
        wait_bytes(srecv.at[index], srecv_sem.at[index])
        wait_bytes(ssend.at[index], ssend_sem.at[index])
        return squares + srecv[index][:, 0:1]

    for g in range(AHEAD):
        issue_weights(jnp.int32(g))

    nstage[...] = jnp.zeros_like(nstage)
    tile[...] = jnp.zeros_like(tile)
    vals[...] = tokens_ref[...].astype(jnp.float32)

    def layer_step(layer, carry):
        load_down(layer, 0, 0)
        load_down(layer, 1, 1)
        values = vals[...]
        squares = add_over_rows(2 * layer, jnp.sum(values * values, axis=1, keepdims=True))
        scale = lax.rsqrt(squares / model_width + norm_eps)
        normed = values * scale * (1.0 + pre_ref[layer])
        width = 2 * rows
        for q in range(own_width // width):
            nstage[q, :, 0:width] = normed[:, q * width : (q + 1) * width].astype(jnp.bfloat16)

        here = offset((c * (cols // 2) + y * planes + z) * own_tokens, own_tokens)
        lines = pl.ds(here, own_tokens)

        half_here = pl.ds(offset(c * half, half), half)

        def scatter(i, carry):
            other = rem(2 * z + y + i, cols // 2)
            send(
                nstage.at[other],
                nrecv.at[0, lines, :],
                nsend_sem.at[0],
                nrecv_sem.at[0],
                (x, other * 2 + c),
            )
            return carry

        lax.fori_loop(1, cols // 2, scatter, 0)
        nrecv[0, lines, :] = nstage[z * 2 + y]
        most = nrecv.at[0, pl.ds(0, half - own_tokens), :]
        wait_bytes(most, nrecv_sem.at[0])
        part = nrecv.at[0, half_here, :]
        for slot, to in enumerate(
            (place(x, z, y, 1 - c), place(1 - x, z, y, c), place(x, z, 1 - y, c))
        ):
            send(
                part,
                nrecv.at[slot, half_here, :],
                nsend_sem.at[1 + slot],
                nrecv_sem.at[1 + slot],
                to,
            )
        for slot in (1, 2):
            wait_bytes(part, nrecv_sem.at[1 + slot])
            send(
                nrecv.at[slot, half_here, :],
                nrecv.at[slot, half_here, :],
                nsend_sem.at[3 + slot],
                nrecv_sem.at[3 + slot],
                place(x, z, y, 1 - c),
            )
        for i in (1, 4, 5):
            wait_bytes(part, nrecv_sem.at[i])
        wait_bytes(most, nsend_sem.at[0])
        for i in range(1, 6):
            wait_bytes(part, nsend_sem.at[i])
        for s in range(2):
            lhs[s, :, 0:kpad] = nrecv[0]
            lhs[s, :, kpad : 2 * kpad] = nrecv[1 + s]

        def unit_step(u, carry):
            g = layer * units + u
            slot = rem(u, 2)

            @pl.when(u < units)
            def _():
                issue_if(g + AHEAD + EXTRA * layer)
                wait_bytes(wbuf.at[g], wrecv_sem.at[g])
                load_tile(g, slot)

            v = u - LAG

            @pl.when(v >= 0)
            def _():
                d, own, j, s = unit_of(v)
                wait_bytes(yrecv.at[v], yrecv_sem.at[v])
                summed = acc[rem(v, acc_slots)] + yrecv[v].astype(jnp.float32)
                relayed = inner * div(d, 2)

                @pl.when(own == 0)
                def _():
                    far = div(d + 1, 3)
                    sent = 3 * j + (1 - inner) * (3 - d) + inner * far * (4 - d)
                    out = rem(sent, slots)

                    @pl.when(sent >= slots)
                    def _():
                        wait_bytes(zsend.at[out], zsend_sem.at[out])

                    @pl.when(relayed == 0)
                    def _():
                        zsend[out] = summed.astype(jnp.bfloat16)

                    @pl.when(relayed == 1)
                    def _():
                        at = d * chunks + j
                        wait_bytes(zrecv.at[at], zrecv_sem.at[at])
                        zsend[out] = (summed + zrecv[at].astype(jnp.float32)).astype(jnp.bfloat16)

                    kind = (1 - inner) * (d - 1 + div(d, 2)) + inner * far
                    at = kind * chunks + j
                    send(
                        zsend.at[out],
                        zrecv.at[at],
                        zsend_sem.at[out],
                        zrecv_sem.at[at],
                        place(x, plane_of(1 - inner + inner * d), y, c),
                    )

                @pl.when(own == 1)
                def _():
                    whole = summed
                    for i in range(2):
                        at = i * chunks + j
                        wait_bytes(zrecv.at[at], zrecv_sem.at[at])
                        whole = whole + zrecv[at].astype(jnp.float32)
                    gate, up_proj = whole[:, :LANES], whole[:, LANES:]
                    hidden[:, pl.ds(offset(j * LANES, LANES), LANES)] = (
                        jax.nn.gelu(gate, approximate=True) * up_proj
                    ).astype(jnp.bfloat16)

            @pl.when(u < units)
            def _():
                s = unit_of(u)[3]
                wait_tile(slot)
                part = jnp.dot(lhs[s], tile[slot], preferred_element_type=jnp.float32)
                out = rem(u, slots)

                @pl.when(u >= slots)
                def _():
                    wait_bytes(ysend.at[out], ysend_sem.at[out])

                ysend[out] = part[:, 2 * LANES :].astype(jnp.bfloat16)
                acc[rem(u, acc_slots)] = part[:, : 2 * LANES]
                send(
                    ysend.at[out],
                    yrecv.at[u],
                    ysend_sem.at[out],
                    yrecv_sem.at[u],
                    place(rem(x + s, 2), z, rem(y + 1 - s, 2), c),
                )

            return carry

        lax.fori_loop(0, units + LAG, unit_step, 0)
        for out in range(min(slots, units)):
            wait_bytes(ysend.at[out], ysend_sem.at[out])
        for out in range(min(slots, units - chunks)):
            wait_bytes(zsend.at[out], zsend_sem.at[out])

        own_half = pl.ds(offset(c * half, half), half)
        far_half = pl.ds(offset((1 - c) * half, half), half)
        own_quarter = pl.ds(offset(y * quarter, quarter), quarter)
        far_quarter = pl.ds(offset((1 - y) * quarter, quarter), quarter)
        own_lines = pl.ds(offset(z * own_tokens, own_tokens), own_tokens)

        def multiply(k):
            slot = k % 2
            wait_bytes(dtile.at[slot], dtile_sem.at[slot])
            csend[k] = jnp.dot(
                hidden[far_half, :], dtile[slot], preferred_element_type=jnp.float32
            ).astype(jnp.bfloat16)
            send(
                csend.at[k], crecv.at[k], bsend_sem.at[0, k], brecv_sem.at[0, k], place(x, z, y, 1 - c)
            )
            bacc[k] = jnp.dot(hidden[own_half, :], dtile[slot], preferred_element_type=jnp.float32)
            if k + 2 < steps:
                load_down(layer, k + 2, slot)

        to_x, to_y = place(1 - x, z, y, c), place(x, z, 1 - y, c)

        def over_first(k):
            wait_bytes(crecv.at[k], brecv_sem.at[0, k])
            summed = bacc[k] + crecv[k].astype(jnp.float32)
            i = k // 2
            if k % 2 == 0:
                bacc[k, :, 0:piece] = summed[:, :piece]
                xs[i] = summed[:, piece:].astype(jnp.bfloat16)
                send(xs.at[i], xr.at[i], bsend_sem.at[1, k], brecv_sem.at[1, k], to_x)
            else:
                bacc[k] = summed
                ys[i] = bacc[k, far_quarter, :].astype(jnp.bfloat16)
                send(ys.at[i], yr.at[i], bsend_sem.at[1, k], brecv_sem.at[1, k], to_y)

        def over_second(k):
            i = k // 2
            if k % 2 == 0:
                wait_bytes(xr.at[i], brecv_sem.at[1, k])
                bacc[k, :, 0:piece] = bacc[k, :, 0:piece] + xr[i].astype(jnp.float32)
                qs[k] = bacc[k, far_quarter, 0:piece].astype(jnp.bfloat16)
                bacc[k, 0:quarter, 0:piece] = bacc[k, own_quarter, 0:piece]
                send(qs.at[k], qr.at[k], bsend_sem.at[2, k], brecv_sem.at[2, k], to_y)
            else:
                wait_bytes(yr.at[i], brecv_sem.at[1, k])
                summed = bacc[k, own_quarter, :] + yr[i].astype(jnp.float32)
                qs[k] = summed[:, piece:].astype(jnp.bfloat16)
                bacc[k, 0:quarter, 0:piece] = summed[:, :piece]
                send(qs.at[k], qr.at[k], bsend_sem.at[2, k], brecv_sem.at[2, k], to_x)

        def over_z(k):
            wait_bytes(qr.at[k], brecv_sem.at[2, k])
            summed = bacc[k, 0:quarter, 0:piece] + qr[k].astype(jnp.float32)
            bacc[k, 0:quarter, 0:piece] = summed
            zs[k] = summed.astype(jnp.bfloat16)
            for shift in range(1, planes):
                pz = rem(z + shift, planes)
                send(
                    zs.at[k, pl.ds(offset(pz * own_tokens, own_tokens), own_tokens), :],
                    zr.at[k, shift - 1],
                    bsend_sem.at[2 + shift, k],
                    brecv_sem.at[2 + shift, k],
                    place(x, pz, y, c),
                )

        def finish(k):
            total = bacc[k, own_lines, 0:piece]
            for shift in range(1, planes):
                wait_bytes(zr.at[k, shift - 1], brecv_sem.at[2 + shift, k])
                total = total + zr[k, shift - 1].astype(jnp.float32)
            branch[:, k * piece : (k + 1) * piece] = total

        stages = (multiply, over_first, over_second, over_z, finish)
        for t in range(steps + len(stages) - 1):
            for lag, stage in enumerate(stages):
                if 0 <= t - lag < steps:
                    stage(t - lag)
            if t < EXTRA:
                issue_if((layer + 1) * units + AHEAD + EXTRA * layer + t)
        for t in range(steps + len(stages) - 1, EXTRA):
            issue_if((layer + 1) * units + AHEAD + EXTRA * layer + t)
        for k in range(steps):
            wait_bytes(csend.at[k], bsend_sem.at[0, k])
            wait_bytes((xs, ys)[k % 2].at[k // 2], bsend_sem.at[1, k])
            wait_bytes(qs.at[k], bsend_sem.at[2, k])
            for shift in range(1, planes):
                wait_bytes(zr.at[k, shift - 1], bsend_sem.at[2 + shift, k])

        summed = branch[...]
        squares = add_over_rows(2 * layer + 1, jnp.sum(summed * summed, axis=1, keepdims=True))
        scale = lax.rsqrt(squares / model_width + norm_eps)
        current = (vals[...] + summed * scale * (1.0 + post_ref[layer])).astype(jnp.bfloat16)
        vals[...] = current.astype(jnp.float32)
        out_ref[...] = current
        return carry

    lax.fori_loop(0, layers, layer_step, 0)

    def drain(g, carry):
        wait_bytes(wbuf.at[g], wsend_sem.at[g])
        return carry

    lax.fori_loop(0, total_units, drain, 0)


def fused(row_count, col_count, tokens, pre_gain, post_gain, gate_weight, up_weight, down_weight):
    planes = col_count // 4
    own_tokens, own_width = tokens.shape
    layers, rows, _ = gate_weight.shape
    block = down_weight.shape[1]
    chunks = block // LANES
    units = planes * chunks
    total_units = layers * units
    every = col_count * own_tokens
    kpad = -(-2 * rows // LANES) * LANES
    piece = max(w for w in (128, 256, 384) if own_width % w == 0)
    steps = own_width // piece
    half = every // 2
    quarter = half // 2
    slots = 4
    bf16, f32 = jnp.bfloat16, jnp.float32
    dma = pltpu.SemaphoreType.DMA
    vmem = pl.BlockSpec(memory_space=pltpu.VMEM)
    hbm = pl.BlockSpec(memory_space=pl.ANY)
    scratch = [
        pltpu.VMEM((own_tokens, own_width), f32),
        pltpu.VMEM((2 * layers, own_tokens, LANES), f32),
        pltpu.VMEM((2 * layers, own_tokens, LANES), f32),
        pltpu.VMEM((own_width // (2 * rows), own_tokens, kpad), bf16),
        pltpu.VMEM((3, every, kpad), bf16),
        pltpu.VMEM((2, every, 2 * kpad), bf16),
        pltpu.VMEM((2, 2 * kpad, 4 * LANES), bf16),
        pltpu.VMEM((LAG + 1, every, 2 * LANES), f32),
        pltpu.VMEM((slots, every, 2 * LANES), bf16),
        pltpu.VMEM((units, every, 2 * LANES), bf16),
        pltpu.VMEM((slots, every, 2 * LANES), bf16),
        pltpu.VMEM((planes * chunks, every, 2 * LANES), bf16),
        pltpu.VMEM((every, block), bf16),
        pltpu.VMEM((2, block, 2 * piece), bf16),
        pltpu.VMEM((steps, half, 2 * piece), bf16),
        pltpu.VMEM((steps, half, 2 * piece), bf16),
        pltpu.VMEM((steps, half, 2 * piece), f32),
        pltpu.VMEM((-(-steps // 2), half, piece), bf16),
        pltpu.VMEM((-(-steps // 2), half, piece), bf16),
        pltpu.VMEM((-(-steps // 2), quarter, 2 * piece), bf16),
        pltpu.VMEM((-(-steps // 2), quarter, 2 * piece), bf16),
        pltpu.VMEM((steps, quarter, piece), bf16),
        pltpu.VMEM((steps, quarter, piece), bf16),
        pltpu.VMEM((steps, quarter, piece), bf16),
        pltpu.VMEM((steps, planes - 1, own_tokens, piece), bf16),
        pltpu.VMEM((own_tokens, own_width), f32),
        dma((2 * layers,)),
        dma((2 * layers,)),
        dma((6,)),
        dma((6,)),
        dma((total_units,)),
        dma((total_units,)),
        dma((2,)),
        dma((slots,)),
        dma((units,)),
        dma((slots,)),
        dma((planes * chunks,)),
        dma((2,)),
        dma((2 + planes, steps)),
        dma((2 + planes, steps)),
    ]
    out, _ = pl.pallas_call(
        functools.partial(fused_kernel, (layers, planes, chunks, steps)),
        out_shape=(
            jax.ShapeDtypeStruct(tokens.shape, bf16),
            jax.ShapeDtypeStruct((total_units, 3, rows, 4 * LANES), bf16),
        ),
        in_specs=[vmem, vmem, vmem, hbm, hbm, hbm],
        out_specs=(vmem, hbm),
        scratch_shapes=scratch,
        compiler_params=pltpu.CompilerParams(
            collective_id=0, has_side_effects=True, vmem_limit_bytes=64 * 1024 * 1024
        ),
        name="blocks",
    )(tokens, pre_gain[:, None, :], post_gain[:, None, :], gate_weight, up_weight, down_weight)
    return out


def activate(gate, up_proj):
    return (jax.nn.gelu(gate, approximate=True) * up_proj).astype(jnp.bfloat16)


def make_on_device(row_count, col_count):
    planes = 4 if col_count % 4 == 0 else 1
    inner = col_count // planes
    members = row_count * inner

    def swap(array, row_bits, plane_bits, seat_bits):
        pairs = []
        for row in range(row_count):
            for plane in range(planes):
                for seat in range(inner):
                    source = row * col_count + plane * inner + seat
                    target = (
                        (row ^ row_bits) * col_count
                        + (plane ^ plane_bits) * inner
                        + (seat ^ seat_bits)
                    )
                    pairs.append((source, target))
        return lax.ppermute(array, AXES, pairs)

    def sum_over_rows(array):
        total = array
        for bits in range(1, row_count):
            total = total + swap(array, bits, 0, 0)
        return total

    def on_device(tokens, pre_gain, post_gain, gate_weight, up_weight, down_weight):
        layer_count = gate_weight.shape[0]
        own_tokens, own_width = tokens.shape
        model_width = own_width * row_count
        stored_rows = gate_weight.shape[1]
        block_width = gate_weight.shape[2] // (row_count * col_count)
        plane_width = own_width // planes
        row = lax.axis_index("row")
        col = lax.axis_index("col")
        plane = col // inner
        seat = col % inner
        member = row * inner + seat

        def weight_chunk(layer_index, plane_bits, after):
            chunk_plane = plane ^ plane_bits
            if after is not None:
                chunk_plane, _ = lax.optimization_barrier((chunk_plane, after))
            held = jnp.zeros((members, stored_rows, 2 * block_width), jnp.bfloat16)
            for bits in range(members):
                row_bits, seat_bits = bits // inner, bits % inner
                start = (
                    (row ^ row_bits) * col_count + chunk_plane * inner + (seat ^ seat_bits)
                ) * block_width
                gate_part, up_part = (
                    lax.dynamic_slice(
                        weight, (layer_index, 0, start), (1, stored_rows, block_width)
                    )
                    for weight in (gate_weight, up_weight)
                )
                block = jnp.concatenate((gate_part, up_part), axis=2)
                if bits:
                    block = swap(block, row_bits, 0, seat_bits)
                held = lax.dynamic_update_slice(held, block, (member ^ bits, 0, 0))
            return held.reshape(members * stored_rows, 2 * block_width)

        def gather_plane(normed):
            parts = normed.reshape(own_tokens, planes, plane_width).transpose(1, 0, 2)
            held = jnp.zeros((planes, own_tokens, plane_width), jnp.bfloat16)
            for bits in range(planes):
                part = lax.dynamic_slice(
                    parts, (plane ^ bits, 0, 0), (1, own_tokens, plane_width)
                )
                if bits:
                    part = swap(part, 0, bits, 0)
                held = lax.dynamic_update_slice(held, part, (plane ^ bits, 0, 0))
            pieces = [held]
            for bits in range(1, row_count):
                pieces.append(swap(held, bits, 0, 0))
            rows = jnp.zeros((row_count,) + held.shape, jnp.bfloat16)
            for bits in range(row_count):
                rows = lax.dynamic_update_slice(rows, pieces[bits][None], (row ^ bits, 0, 0, 0))
            whole = rows.transpose(1, 2, 0, 3).reshape(
                planes, 1, own_tokens, row_count * plane_width
            )
            bit = inner // 2
            order = [0]
            blocks = whole
            while bit:
                blocks = jnp.concatenate((blocks, swap(blocks, 0, 0, bit)), axis=1)
                order = order + [seat_bits ^ bit for seat_bits in order]
                bit //= 2
            return blocks.reshape(planes * inner * own_tokens, row_count * plane_width), order

        def scatter_branch(branch):
            bit = 1
            halved_rows = False
            while bit < inner or not halved_rows:
                if bit < inner:
                    half = branch.shape[1] // 2
                    away = branch[:, half:].astype(jnp.bfloat16)
                    branch = branch[:, :half] + swap(away, 0, 0, bit).astype(jnp.float32)
                    bit *= 2
                if not halved_rows:
                    split = [
                        branch[..., i * own_width : (i + 1) * own_width]
                        for i in range(row_count)
                    ]

                    def part_of(wanted):
                        chosen = split[0]
                        for i in range(1, row_count):
                            chosen = jnp.where(wanted == i, split[i], chosen)
                        return chosen

                    total = part_of(row)
                    for bits in range(1, row_count):
                        away = part_of(row ^ bits).astype(jnp.bfloat16)
                        total = total + swap(away, bits, 0, 0).astype(jnp.float32)
                    branch = total
                    halved_rows = True
            branch = branch.reshape(planes, own_tokens, own_width)
            total = lax.dynamic_slice(branch, (plane, 0, 0), (1, own_tokens, own_width))
            for bits in range(1, planes):
                away = lax.dynamic_slice(
                    branch, (plane ^ bits, 0, 0), (1, own_tokens, own_width)
                ).astype(jnp.bfloat16)
                total = total + swap(away, 0, bits, 0).astype(jnp.float32)
            return total[0]

        current = tokens
        landed = []
        for layer_index in range(layer_count):
            values = current.astype(jnp.float32)
            squares = sum_over_rows(jnp.sum(values * values, axis=1, keepdims=True))
            scale_pre = lax.rsqrt(squares / model_width + norm_eps)
            normed = (values * scale_pre * (1.0 + pre_gain[layer_index])[None, :]).astype(
                jnp.bfloat16
            )
            gathered, order = gather_plane(normed)
            arrived = []
            for bits in reversed(range(planes)):
                after = landed[-2] if len(landed) > 1 else gathered if landed else None
                chunk = weight_chunk(layer_index, bits, after)
                landed.append(chunk)
                part = jnp.dot(gathered, chunk, preferred_element_type=jnp.float32)
                if bits:
                    part = swap(part.astype(jnp.bfloat16), 0, bits, 0)
                arrived.append(part)
            summed = arrived[-1]
            for part in arrived[:-1]:
                summed = summed + part.astype(jnp.float32)
            hidden = activate(summed[:, :block_width], summed[:, block_width:])
            branch = jnp.dot(hidden, down_weight[layer_index], preferred_element_type=jnp.float32)
            branch = branch.reshape(planes, inner, own_tokens, model_width)
            branch = scatter_branch(branch)
            branch_squares = sum_over_rows(jnp.sum(branch * branch, axis=1, keepdims=True))
            scale_post = lax.rsqrt(branch_squares / model_width + norm_eps)
            post = branch * scale_post * (1.0 + post_gain[layer_index])[None, :]
            current = (values + post).astype(jnp.bfloat16)
        return current

    return on_device


def solution(mesh):
    in_specs = (
        P("col", "row"),
        P(None, "row"),
        P(None, "row"),
        P(None, ("row", "col"), None),
        P(None, ("row", "col"), None),
        P(None, ("row", "col"), None),
    )
    out_specs = P("col", "row")
    sizes = mesh.shape["row"], mesh.shape["col"]
    permuted = make_on_device(*sizes)

    def on_device(*arrays):
        tokens, _, _, gate_weight, _, down_weight = arrays
        if fits(*sizes, (tokens.shape, gate_weight.shape, down_weight.shape)):
            return fused(*sizes, *arrays)
        return permuted(*arrays)

    return jax.shard_map(
        on_device, mesh=mesh, in_specs=in_specs, out_specs=out_specs, check_vma=False
    )
```
